256 devices in a mesh: gx: 8 (over z), gy: 32 (over y, x, core).
Axes of the slice: x: 4, y: 4, z: 8, core: 2. Of those that a mesh axis runs over, the one named last changes fastest.
Arguments:
- substrates: float32 [8, 512, 512, 128], P(None, 'gx', 'gy'), may hold values from 0 to 2
- uptake: float32 [512, 512, 128], P('gx', 'gy'), may hold values from 0.5 to 2
- diffusion: float32 [8], replicated, may hold values from 0.1 to 0.15
- decay_rate: float32 [8], replicated, may hold values from 0.01 to 0.1
Outputs:
- advanced: float32 [8, 512, 512, 128], P(None, 'gx', 'gy')
The draws below stay inside these ranges and needn't reach their ends.
All inputs are finite; a program needn't handle non-finite values.
Results may differ from the reference program's by a relative error of at most 0.00002.
Values sent between devices are 32-bit elements; how exact they have to be, the bound alone decides.
A program may use at most 128 MiB of HBM per device.

```python
import math
import jax
import jax.numpy as jnp

S = 8
CX = 64
CY = 16
CZ = 128
SUBSTEPS = 4
NX = 512
NY = 512


def draw_substrates(key, part):
    first_key, second_key, third_key = jax.random.split(jax.random.fold_in(key, 17), 3)
    grid_shape = (S, NX, NY, CZ)
    x_local = jnp.arange(NX) % CX
    y_local = jnp.arange(NY) % CY
    x_band = (x_local < 4) | (x_local >= CX - 4)
    y_band = (y_local < 4) | (y_local >= CY - 4)
    in_band = (x_band[:, None] | y_band[None, :])[None, :, :, None]
    coin_flips = jax.random.randint(first_key, grid_shape, 0, 2).astype(jnp.float32)
    jitter_values = jax.random.uniform(second_key, grid_shape, jnp.float32)
    inside_draw = jax.random.uniform(third_key, grid_shape, jnp.float32)
    edge_values = 1.6 * coin_flips + 0.4 * jitter_values
    inside_values = 0.4 + 0.4 * inside_draw
    return jnp.where(in_band, edge_values, inside_values).astype(jnp.float32)


def block_scale(own_key, extent, cuts, least, largest):
    factor_of, own = 1.0, jax.random.fold_in(own_key, 6)
    for dim, blocks in cuts:
        steps = jnp.exp(jax.random.uniform(jax.random.fold_in(own, dim), (blocks,), jnp.float32, least / len(cuts), largest / len(cuts)))
        factor_of = factor_of * jnp.repeat(steps, extent[dim] // blocks).reshape([-1 if axis == dim else 1 for axis in range(len(extent))])
    return factor_of


def setup_inputs(seed: int = 0) -> dict:
    splits = jax.random.split(jax.random.key(seed), 5)
    return {
        "substrates": draw_substrates(jax.random.fold_in(splits[4], 71), 0),
        "uptake": jnp.clip(jnp.exp(math.log(2.0) - 1.3862944 * jax.random.uniform(splits[1], (NX, NY, CZ), jnp.float32) ** block_scale(splits[1], (NX, NY, CZ), ((0, 8), (1, 32)), -0.2, 0.2)), 0.5, 2.0),
        "diffusion": jnp.clip(jnp.exp(jax.random.uniform(splits[2], (S,), jnp.float32, math.log(0.1), math.log(0.15))), 0.1, 0.15),
        "decay_rate": jnp.clip(jnp.exp(jax.random.uniform(splits[3], (S,), jnp.float32, math.log(0.01), math.log(0.1))), 0.01, 0.1),
    }


def advance(concentration, uptake, diffuse, decays):
    laplace = jnp.roll(concentration, -1, 1) + jnp.roll(concentration, 1, 1)
    laplace = laplace + jnp.roll(concentration, -1, 2) + jnp.roll(concentration, 1, 2)
    laplace = laplace + jnp.roll(concentration, -1, 3) + jnp.roll(concentration, 1, 3)
    laplace = laplace - 6.0 * concentration
    return concentration + diffuse * laplace - decays * uptake[None] * concentration


def reference(substrates, uptake, diffusion, decay_rate):
    diffuse = diffusion[:, None, None, None]
    decays = decay_rate[:, None, None, None]
    concentration = substrates
    for substep in range(SUBSTEPS):
        concentration = advance(concentration, uptake, diffuse, decays)
    return concentration
```

```python
import functools

import jax
import jax.numpy as jnp
from jax import lax
from jax.experimental import pallas as pl
from jax.experimental.pallas import tpu as pltpu
from jax.sharding import PartitionSpec as P

S, CX, CY, CZ = 8, 64, 16, 128
W = 2
PX, PY = CX + 2 * W, CY + 2 * W
MESH = pl.DeviceIdType.MESH

FACES = ((0, 1), (0, -1), (1, 0), (-1, 0))
CORNERS = ((1, 1), (1, -1), (-1, 1), (-1, -1))


def sent(step, size, width, around):
    if step == 0:
        return pl.ds(around, size), pl.ds(around, size)
    if step > 0:
        return pl.ds(around + size - width, width), pl.ds(around - width, width)
    return pl.ds(around, width), pl.ds(around + size, width)


def substep(src, dst, up, rate, decay, planes, group, starts, up_at, dst_at):
    stay = 1.0 - 6.0 * rate

    def body(g, carry):
        for n in range(group):
            i = g * group + n
            for j in starts:
                center = src[i + 1, j + 1 : j + 9, :]
                total = src[i + 1, j : j + 8, :] + src[i + 1, j + 2 : j + 10, :]
                total = total + (src[i, j + 1 : j + 9, :] + src[i + 2, j + 1 : j + 9, :])
                total = total + (pltpu.roll(center, 1, 1) + pltpu.roll(center, CZ - 1, 1))
                keep = stay - decay * up[i + up_at, j + up_at : j + up_at + 8, :]
                dst[i + dst_at, j + dst_at : j + dst_at + 8, :] = keep * center + rate * total
        return carry

    lax.fori_loop(0, planes // group, body, 0)


def kernel(
    nx, ny, x_hbm, u_hbm, d_hbm, k_hbm, out, d_ref, k_ref,
    first, second, half, up, load_sem, send_sem, recv_sem, corner_send, corner_recv, up_send, up_recv,
):
    gx, gy = lax.axis_index("gx"), lax.axis_index("gy")

    def device(step):
        return (lax.rem(gx + step[0] + nx, nx), lax.rem(gy + step[1] + ny, ny))

    def load(s):
        return pltpu.make_async_copy(
            x_hbm.at[s], first.at[s, pl.ds(W, CX), pl.ds(W, CY)], load_sem.at[s]
        )

    load_up = pltpu.make_async_copy(
        u_hbm, up.at[pl.ds(1, CX), pl.ds(1, CY)], load_sem.at[S]
    )
    for s in range(S):
        load(s).start()
    load_up.start()
    load_d = pltpu.make_async_copy(d_hbm, d_ref, load_sem.at[S + 1])
    load_k = pltpu.make_async_copy(k_hbm, k_ref, load_sem.at[S + 2])
    load_d.start()
    load_k.start()

    barrier = pltpu.get_barrier_semaphore()
    for step in FACES + CORNERS:
        pl.semaphore_signal(barrier, inc=1, device_id=device(step), device_id_type=MESH)
    pl.semaphore_wait(barrier, len(FACES + CORNERS))

    def face(buffer, r, s, d):
        step = FACES[d]
        (x_from, x_to), (y_from, y_to) = sent(step[0], CX, W, W), sent(step[1], CY, W, W)
        return pltpu.make_async_remote_copy(
            src_ref=buffer.at[s, x_from, y_from], dst_ref=buffer.at[s, x_to, y_to],
            send_sem=send_sem.at[r, s, d], recv_sem=recv_sem.at[r, s, d],
            device_id=device(step), device_id_type=MESH,
        )

    def corner(buffer, which, slot, d):
        step = CORNERS[d]
        (x_from, x_to), (y_from, y_to) = sent(step[0], CX, 1, W), sent(step[1], CY, 1, W)
        return pltpu.make_async_remote_copy(
            src_ref=buffer.at[which, x_from, y_from], dst_ref=buffer.at[which, x_to, y_to],
            send_sem=corner_send.at[slot, d], recv_sem=corner_recv.at[slot, d],
            device_id=device(step), device_id_type=MESH,
        )

    def up_face(d):
        step = FACES[d]
        (x_from, x_to), (y_from, y_to) = sent(step[0], CX, 1, 1), sent(step[1], CY, 1, 1)
        return pltpu.make_async_remote_copy(
            src_ref=up.at[x_from, y_from], dst_ref=up.at[x_to, y_to],
            send_sem=up_send.at[d], recv_sem=up_recv.at[d],
            device_id=device(step), device_id_type=MESH,
        )

    for s in range(S):
        load(s).wait()
    load_up.wait()
    load_d.wait()
    load_k.wait()
    whole = pl.ds(0, S)
    for d in range(4):
        face(first, 0, 0, d).start()
    for d in range(4):
        up_face(d).start()
    for d in range(4):
        corner(first, whole, S, d).start()

    def send(s, carry):
        for d in range(4):
            face(first, 0, s, d).start()
        return carry

    lax.fori_loop(1, S, send, 0)

    for d in range(4):
        up_face(d).wait_recv()
    for d in range(4):
        corner(first, whole, S, d).wait_recv()

    outer = (0, 8, CY + 2 - 8)
    inner = (0, 8)

    def advance(buffer, s, result, at):
        rate, decay = d_ref[s], k_ref[s]
        substep(buffer.at[s], half, up, rate, decay, CX + 2, 6, outer, 0, 0)
        substep(half, result.at[s], up, rate, decay, CX, 8, inner, 1, at)

    def round_one(s, carry):
        for d in range(4):
            face(first, 0, s, d).wait_recv()
        advance(first, s, second, W)
        for d in range(4):
            corner(second, pl.ds(s, 1), s, d).start()
        for d in range(4):
            face(second, 1, s, d).start()
        return carry

    lax.fori_loop(0, S, round_one, 0)

    def round_two(s, carry):
        for d in range(4):
            face(second, 1, s, d).wait_recv()
        for d in range(4):
            corner(second, pl.ds(s, 1), s, d).wait_recv()
        advance(second, s, out, 0)
        return carry

    lax.fori_loop(0, S, round_two, 0)

    def drain(s, carry):
        for d in range(4):
            face(first, 0, s, d).wait_send()
            face(second, 1, s, d).wait_send()
            corner(second, pl.ds(s, 1), s, d).wait_send()
        return carry

    lax.fori_loop(0, S, drain, 0)
    for d in range(4):
        up_face(d).wait_send()
        corner(first, whole, S, d).wait_send()


def solution(mesh):
    nx, ny = mesh.shape["gx"], mesh.shape["gy"]

    def local(*arrays):
        arrays = [pltpu.with_memory_space_constraint(a, pltpu.HBM) for a in arrays]
        return pl.pallas_call(
            functools.partial(kernel, nx, ny),
            out_shape=jax.ShapeDtypeStruct((S, CX, CY, CZ), jnp.float32),
            in_specs=[pl.BlockSpec(memory_space=pltpu.HBM)] * 4,
            out_specs=pl.BlockSpec(memory_space=pltpu.VMEM),
            scratch_shapes=[
                pltpu.SMEM((S,), jnp.float32),
                pltpu.SMEM((S,), jnp.float32),
                pltpu.VMEM((S, PX, PY, CZ), jnp.float32),
                pltpu.VMEM((S, PX, PY, CZ), jnp.float32),
                pltpu.VMEM((CX + 2, CY + 2, CZ), jnp.float32),
                pltpu.VMEM((CX + 2, CY + 2, CZ), jnp.float32),
                pltpu.SemaphoreType.DMA((S + 3,)),
                pltpu.SemaphoreType.DMA((2, S, 4)),
                pltpu.SemaphoreType.DMA((2, S, 4)),
                pltpu.SemaphoreType.DMA((S + 1, 4)),
                pltpu.SemaphoreType.DMA((S + 1, 4)),
                pltpu.SemaphoreType.DMA((4,)),
                pltpu.SemaphoreType.DMA((4,)),
            ],
            compiler_params=pltpu.CompilerParams(
                collective_id=0, has_side_effects=True, vmem_limit_bytes=40 << 20
            ),
        )(*arrays)

    placed = (P(None, "gx", "gy", None), P("gx", "gy", None), P(), P())
    return jax.shard_map(
        local, mesh=mesh, in_specs=placed, out_specs=P(None, "gx", "gy", None), check_vma=False
    )
```

```python
import functools

import jax
import jax.numpy as jnp
from jax import lax
from jax.experimental import pallas as pl
from jax.experimental.pallas import tpu as pltpu
from jax.sharding import PartitionSpec as P

S, CX, CY, CZ = 8, 64, 16, 128
W = 2
PX, PY = CX + 2 * W, CY + 2 * W
MESH = pl.DeviceIdType.MESH

FACES = ((0, 1), (0, -1), (1, 0), (-1, 0))
CORNERS = ((1, 1), (1, -1), (-1, 1), (-1, -1))


def sent(step, size, width, around):
    if step == 0:
        return pl.ds(around, size), pl.ds(around, size)
    if step > 0:
        return pl.ds(around + size - width, width), pl.ds(around - width, width)
    return pl.ds(around, width), pl.ds(around + size, width)


def neighbours_in_z(z_sum, center, by_matmul):
    cells = center[:by_matmul].reshape(by_matmul * 8, CZ)
    high = cells.astype(jnp.bfloat16)
    low = (cells - high.astype(jnp.float32)).astype(jnp.bfloat16)
    first = jnp.dot(
        jnp.concatenate([high, low], axis=1), z_sum, preferred_element_type=jnp.float32
    ).reshape(by_matmul, 8, CZ)
    rest = center[by_matmul:]
    return jnp.concatenate([first, pltpu.roll(rest, 1, 2) + pltpu.roll(rest, CZ - 1, 2)], axis=0)


def substep(src, dst, up, z_sum, rate, decay, planes, starts, up_at, dst_at):
    stay = 1.0 - 6.0 * rate
    by_matmul = planes * 2 // 3
    for j in starts:
        center = src[1 : planes + 1, j + 1 : j + 9, :]
        total = neighbours_in_z(z_sum, center, by_matmul)
        total = total + (src[1 : planes + 1, j : j + 8, :] + src[1 : planes + 1, j + 2 : j + 10, :])
        total = total + (src[0:planes, j + 1 : j + 9, :] + src[2 : planes + 2, j + 1 : j + 9, :])
        keep = stay - decay * up[up_at : planes + up_at, j + up_at : j + up_at + 8, :]
        dst[dst_at : planes + dst_at, j + dst_at : j + dst_at + 8, :] = keep * center + rate * total


def kernel(
    nx, ny, x_hbm, u_hbm, d_hbm, k_hbm, out, d_ref, k_ref,
    first, second, half, up, load_sem, send_sem, recv_sem, corner_send, corner_recv, up_send, up_recv,
):
    gx, gy = lax.axis_index("gx"), lax.axis_index("gy")

    def device(step):
        return (lax.rem(gx + step[0] + nx, nx), lax.rem(gy + step[1] + ny, ny))

    def load(s):
        return pltpu.make_async_copy(
            x_hbm.at[s], first.at[s, pl.ds(W, CX), pl.ds(W, CY)], load_sem.at[s]
        )

    load_up = pltpu.make_async_copy(
        u_hbm, up.at[pl.ds(1, CX), pl.ds(1, CY)], load_sem.at[S]
    )
    for s in range(S):
        load(s).start()
    load_up.start()
    load_d = pltpu.make_async_copy(d_hbm, d_ref, load_sem.at[S + 1])
    load_k = pltpu.make_async_copy(k_hbm, k_ref, load_sem.at[S + 2])
    load_d.start()
    load_k.start()

    barrier = pltpu.get_barrier_semaphore()
    for step in FACES + CORNERS:
        pl.semaphore_signal(barrier, inc=1, device_id=device(step), device_id_type=MESH)
    pl.semaphore_wait(barrier, len(FACES + CORNERS))

    def face(buffer, r, s, d):
        step = FACES[d]
        (x_from, x_to), (y_from, y_to) = sent(step[0], CX, W, W), sent(step[1], CY, W, W)
        return pltpu.make_async_remote_copy(
            src_ref=buffer.at[s, x_from, y_from], dst_ref=buffer.at[s, x_to, y_to],
            send_sem=send_sem.at[r, s, d], recv_sem=recv_sem.at[r, s, d],
            device_id=device(step), device_id_type=MESH,
        )

    def corner(buffer, which, slot, d):
        step = CORNERS[d]
        (x_from, x_to), (y_from, y_to) = sent(step[0], CX, 1, W), sent(step[1], CY, 1, W)
        return pltpu.make_async_remote_copy(
            src_ref=buffer.at[which, x_from, y_from], dst_ref=buffer.at[which, x_to, y_to],
            send_sem=corner_send.at[slot, d], recv_sem=corner_recv.at[slot, d],
            device_id=device(step), device_id_type=MESH,
        )

    def up_face(d):
        step = FACES[d]
        (x_from, x_to), (y_from, y_to) = sent(step[0], CX, 1, 1), sent(step[1], CY, 1, 1)
        return pltpu.make_async_remote_copy(
            src_ref=up.at[x_from, y_from], dst_ref=up.at[x_to, y_to],
            send_sem=up_send.at[d], recv_sem=up_recv.at[d],
            device_id=device(step), device_id_type=MESH,
        )

    for s in range(S):
        load(s).wait()
    load_up.wait()
    load_d.wait()
    load_k.wait()
    whole = pl.ds(0, S)
    for d in range(4):
        face(first, 0, 0, d).start()
    for d in range(4):
        up_face(d).start()
    for d in range(4):
        corner(first, whole, S, d).start()

    def send(s, carry):
        for d in range(4):
            face(first, 0, s, d).start()
        return carry

    lax.fori_loop(1, S, send, 0)

    for d in range(4):
        up_face(d).wait_recv()
    for d in range(4):
        corner(first, whole, S, d).wait_recv()

    apart = lax.rem(
        lax.broadcasted_iota(jnp.int32, (2 * CZ, CZ), 0) - lax.broadcasted_iota(jnp.int32, (2 * CZ, CZ), 1) + CZ, CZ
    )
    z_sum = jnp.where((apart == 1) | (apart == CZ - 1), 1.0, 0.0).astype(jnp.bfloat16)

    outer = (0, 8, CY + 2 - 8)
    inner = (0, 8)

    def advance(buffer, s, result, at):
        rate, decay = d_ref[s], k_ref[s]
        substep(buffer.at[s], half, up, z_sum, rate, decay, CX + 2, outer, 0, 0)
        substep(half, result.at[s], up, z_sum, rate, decay, CX, inner, 1, at)

    def round_one(s, carry):
        for d in range(4):
            face(first, 0, s, d).wait_recv()
        advance(first, s, second, W)
        for d in range(4):
            corner(second, pl.ds(s, 1), s, d).start()
        for d in range(4):
            face(second, 1, s, d).start()
        return carry

    lax.fori_loop(0, S, round_one, 0)

    def round_two(s, carry):
        for d in range(4):
            face(second, 1, s, d).wait_recv()
        for d in range(4):
            corner(second, pl.ds(s, 1), s, d).wait_recv()
        advance(second, s, out, 0)
        return carry

    lax.fori_loop(0, S, round_two, 0)

    def drain(s, carry):
        for d in range(4):
            face(first, 0, s, d).wait_send()
            face(second, 1, s, d).wait_send()
            corner(second, pl.ds(s, 1), s, d).wait_send()
        return carry

    lax.fori_loop(0, S, drain, 0)
    for d in range(4):
        up_face(d).wait_send()
        corner(first, whole, S, d).wait_send()


def solution(mesh):
    nx, ny = mesh.shape["gx"], mesh.shape["gy"]

    def local(*arrays):
        arrays = [pltpu.with_memory_space_constraint(a, pltpu.HBM) for a in arrays]
        return pl.pallas_call(
            functools.partial(kernel, nx, ny),
            out_shape=jax.ShapeDtypeStruct((S, CX, CY, CZ), jnp.float32),
            in_specs=[pl.BlockSpec(memory_space=pltpu.HBM)] * 4,
            out_specs=pl.BlockSpec(memory_space=pltpu.VMEM),
            scratch_shapes=[
                pltpu.SMEM((S,), jnp.float32),
                pltpu.SMEM((S,), jnp.float32),
                pltpu.VMEM((S, PX, PY, CZ), jnp.float32),
                pltpu.VMEM((S, PX, PY, CZ), jnp.float32),
                pltpu.VMEM((CX + 2, CY + 2, CZ), jnp.float32),
                pltpu.VMEM((CX + 2, CY + 2, CZ), jnp.float32),
                pltpu.SemaphoreType.DMA((S + 3,)),
                pltpu.SemaphoreType.DMA((2, S, 4)),
                pltpu.SemaphoreType.DMA((2, S, 4)),
                pltpu.SemaphoreType.DMA((S + 1, 4)),
                pltpu.SemaphoreType.DMA((S + 1, 4)),
                pltpu.SemaphoreType.DMA((4,)),
                pltpu.SemaphoreType.DMA((4,)),
            ],
            compiler_params=pltpu.CompilerParams(
                collective_id=0, has_side_effects=True, vmem_limit_bytes=40 << 20
            ),
        )(*arrays)

    placed = (P(None, "gx", "gy", None), P("gx", "gy", None), P(), P())
    return jax.shard_map(
        local, mesh=mesh, in_specs=placed, out_specs=P(None, "gx", "gy", None), check_vma=False
    )
```

```python
import functools

import jax
import jax.numpy as jnp
from jax import lax
from jax.experimental import pallas as pl
from jax.experimental.pallas import tpu as pltpu
from jax.sharding import PartitionSpec as P

S, CX, CY, CZ = 8, 64, 16, 128
MESH = pl.DeviceIdType.MESH
PASS_ON, PASS_ON_FIRST, SEND_FIRST, BEFORE_EDGES = 1, 7, 2, 2

FIRST, SECOND, HALF, UP = (4, 2), (2, 2), (3, 1), (3, 1)
OUTER, INNER = (-1, 7, 9), (0, 8)


def neighbours_in_z(z_sum, center):
    by_matmul = center.shape[0] * 2 // 3
    cells = center[:by_matmul].reshape(by_matmul * 8, CZ)
    high = cells.astype(jnp.bfloat16)
    low = (cells - high.astype(jnp.float32)).astype(jnp.bfloat16)
    first = jnp.dot(
        jnp.concatenate([high, low], axis=1), z_sum, preferred_element_type=jnp.float32
    ).reshape(by_matmul, 8, CZ)
    rest = center[by_matmul:]
    return jnp.concatenate([first, pltpu.roll(rest, 1, 2) + pltpu.roll(rest, CZ - 1, 2)], axis=0)


def substep(jobs, up, z_sum):
    def at(ref, where, x, n, y):
        return ref.at[pl.ds(x + where[0], n), pl.ds(y + where[1], 8)]

    centers = [at(src, where, x, n, y)[...] for src, where, _, _, x, n, y, _, _ in jobs]
    sums, done = neighbours_in_z(z_sum, jnp.concatenate(centers, axis=0)), 0
    for center, (src, where, dst, to, x, n, y, rate, decay) in zip(centers, jobs, strict=True):
        total = sums[done : done + n]
        done += n
        total = total + (at(src, where, x, n, y - 1)[...] + at(src, where, x, n, y + 1)[...])
        total = total + (at(src, where, x - 1, n, y)[...] + at(src, where, x + 1, n, y)[...])
        keep = (1.0 - 6.0 * rate) - decay * at(up, UP, x, n, y)[...]
        at(dst, to, x, n, y)[...] = keep * center + rate * total


def kernel(
    nx, ny, x_hbm, u_hbm, d_hbm, k_hbm, out, d_ref, k_ref, first, second, half, edge, up,
    load_sem, y_send, y_recv, x_send, x_recv, up_send, up_recv, corner_send, corner_recv, above, below,
):
    gx, gy = lax.axis_index("gx"), lax.axis_index("gy")

    def device(dx, dy):
        return (lax.rem(gx + dx + nx, nx), lax.rem(gy + dy + ny, ny))

    def load(s):
        return pltpu.make_async_copy(x_hbm.at[s], first.at[s, pl.ds(4, CX), pl.ds(2, CY)], load_sem.at[s])

    load_up = pltpu.make_async_copy(u_hbm, up.at[pl.ds(3, CX), pl.ds(1, CY)], load_sem.at[S])
    load_d = pltpu.make_async_copy(d_hbm, d_ref, load_sem.at[S + 1])
    load_k = pltpu.make_async_copy(k_hbm, k_ref, load_sem.at[S + 2])

    is_first, is_last = gx == 0, gx == nx - 1
    barrier = pltpu.get_barrier_semaphore()

    def signal(sem, dx, dy):
        pl.semaphore_signal(sem, inc=1, device_id=device(dx, dy), device_id_type=MESH)

    signal(barrier, 0, 1)
    signal(barrier, 0, -1)
    pl.when(jnp.logical_not(is_last))(lambda: signal(barrier, 1, 0))
    pl.when(is_first)(lambda: signal(barrier, -1, 0))
    for s in range(S):
        load(s).start()
    for copy in (load_up, load_d, load_k):
        copy.start()

    def remote(src, dst, send_sem, recv_sem, to):
        return pltpu.make_async_remote_copy(
            src_ref=src, dst_ref=dst, send_sem=send_sem, recv_sem=recv_sem,
            device_id=to, device_id_type=MESH,
        )

    both = (0, 1)
    pairs = ((0, 0), (0, 1), (1, 0), (1, 1))
    rows = ((16, 0), (2, 18))
    all_s = pl.ds(0, S)

    def y_face(r, s, d):
        buffer, planes = ((first, pl.ds(4, CX)), (second, pl.ds(4, CX - 4)))[r]
        a, b = rows[d]
        return remote(
            buffer.at[s, planes, pl.ds(a, 2)], buffer.at[s, planes, pl.ds(b, 2)],
            y_send.at[r, d], y_recv.at[r, s, d], device(0, 1 - 2 * d),
        )

    def x_face(part, d):
        a, b = ((64, 0), (4, 68))[d]
        r = (pl.ds(2, 2), pl.ds(16, 2), pl.ds(4, 12))[part]
        return remote(
            first.at[all_s, pl.ds(a, 4), r], first.at[all_s, pl.ds(b, 4), r],
            x_send.at[d], x_recv.at[part, d], device(1 - 2 * d, 0),
        )

    def up_y(d):
        a, b = ((16, 0), (1, 17))[d]
        return remote(
            up.at[pl.ds(3, CX), pl.ds(a, 1)], up.at[pl.ds(3, CX), pl.ds(b, 1)],
            up_send.at[0, d], up_recv.at[0, d], device(0, 1 - 2 * d),
        )

    def up_x(d):
        a, b = ((64, 0), (3, 67))[d]
        return remote(
            up.at[pl.ds(a, 3), pl.ds(1, CY)], up.at[pl.ds(b, 3), pl.ds(1, CY)],
            up_send.at[1, d], up_recv.at[1, d], device(1 - 2 * d, 0),
        )

    def corner(kind, side, d):
        to = device(0, 1 - 2 * d)
        sems = corner_send.at[kind], corner_recv.at[kind]
        if kind == 0:
            planes, (a, b) = pl.ds((1, 68)[side], 3), rows[d]
            return remote(first.at[all_s, planes, pl.ds(a, 2)], first.at[all_s, planes, pl.ds(b, 2)], *sems, to)
        if kind == 1:
            planes, (a, b) = pl.ds((1, 67)[side], 2), ((16, 0), (1, 17))[d]
            return remote(up.at[planes, pl.ds(a, 1)], up.at[planes, pl.ds(b, 1)], *sems, to)
        planes, (a, b) = pl.ds((1, 64)[side], 3), rows[d]
        return remote(second.at[all_s, planes, pl.ds(a, 2)], second.at[all_s, planes, pl.ds(b, 2)], *sems, to)

    def corners_arrived(kind):
        ref = (first.at[all_s, pl.ds(0, 12), pl.ds(0, 2)], up.at[pl.ds(0, 8), pl.ds(0, 1)])[kind % 2]
        pltpu.make_async_copy(ref, ref, corner_recv.at[kind]).wait()

    pl.semaphore_wait(barrier, 2 + jnp.where(is_first, 0, 1) + jnp.where(is_last, 1, 0))
    pl.when(jnp.logical_not(is_first))(lambda: signal(above, -1, 0))
    pl.when(is_last)(lambda: signal(below, 1, 0))
    load(0).wait()
    for d in both:
        y_face(0, 0, d).start()
    load_up.wait()
    for d in both:
        up_y(d).start()
    for s in range(1, S):
        load(s).wait()
        for d in both:
            y_face(0, s, d).start()

    def send_along_gx(d):
        up_x(d).start()
        for part in range(3):
            x_face(part, d).start()

    pl.when(jnp.logical_not(is_first))(lambda: send_along_gx(1))
    pl.when(jnp.logical_not(is_last))(lambda: pl.semaphore_wait(above, 1))
    send_along_gx(0)
    load_d.wait()
    load_k.wait()

    apart = lax.rem(
        lax.broadcasted_iota(jnp.int32, (2 * CZ, CZ), 0) - lax.broadcasted_iota(jnp.int32, (2 * CZ, CZ), 1) + CZ, CZ
    )
    z_sum = jnp.where((apart == 1) | (apart == CZ - 1), 1.0, 0.0).astype(jnp.bfloat16)

    def middle(src, where, s, dst, to, x, n):
        rates = d_ref[s], k_ref[s]
        substep([(src.at[s], where, half, HALF, x, n, y, *rates) for y in OUTER], up, z_sum)
        substep([(half, HALF, dst.at[s], to, x + 1, n - 2, y, *rates) for y in INNER], up, z_sum)

    def edges(src, where, dst, to, starts):
        rates = [(d_ref[s], k_ref[s]) for s in range(S)]
        between = [[(edge.at[s, side], (-x, 1)) for side, x in enumerate(starts)] for s in range(S)]
        substep(
            [
                (src.at[s], where, *between[s][side], x, 6, y, *rates[s])
                for s in range(S) for side, x in enumerate(starts) for y in OUTER
            ], up, z_sum,
        )
        substep(
            [
                (*between[s][side], dst.at[s], to, x + 1, 4, y, *rates[s])
                for s in range(S) for side, x in enumerate(starts) for y in INNER
            ], up, z_sum,
        )

    for d in both:
        up_y(d).wait_recv()

    def pass_on():
        for d in both:
            up_x(d).wait_recv()
            x_face(0, d).wait_recv()
            x_face(1, d).wait_recv()
        for kind in both:
            for side, d in pairs:
                corner(kind, side, d).start()

    def send_down_first():
        pl.semaphore_wait(below, 1)
        send_along_gx(1)

    def round_one(s, carry):
        for d in both:
            y_face(0, s, d).wait_recv()
        middle(first, FIRST, s, second, SECOND, 1, CX - 2)
        for d in both:
            y_face(1, s, d).start()
        pl.when(jnp.logical_and(is_first, s == SEND_FIRST))(send_down_first)
        pl.when(s == jnp.where(is_first, PASS_ON_FIRST, PASS_ON))(pass_on)
        return carry

    lax.fori_loop(0, S, round_one, 0)

    def round_two(s, carry):
        for d in both:
            y_face(1, s, d).wait_recv()
        middle(second, SECOND, s, out, (0, 0), 3, CX - 6)

        @pl.when(s == BEFORE_EDGES - 1)
        def _():
            for d in both:
                x_face(2, d).wait_recv()
            corners_arrived(0)
            corners_arrived(1)
            edges(first, FIRST, second, SECOND, (-3, CX - 3))
            for side, d in pairs:
                corner(2, side, d).start()

        return carry

    lax.fori_loop(0, S, round_two, 0)
    corners_arrived(2)
    edges(second, SECOND, out, (0, 0), (-1, CX - 5))

    def sent(ref, sem):
        pltpu.make_async_copy(ref, ref, sem).wait()

    for d in both:
        sent(first.at[all_s, pl.ds(0, CX), pl.ds(0, 2)], y_send.at[0, d])
        sent(second.at[all_s, pl.ds(0, CX - 4), pl.ds(0, 2)], y_send.at[1, d])
        sent(first.at[all_s, pl.ds(0, 4), pl.ds(0, CY)], x_send.at[d])
        up_y(d).wait_send()
        up_x(d).wait_send()
    for kind in range(3):
        sent((first.at[all_s, pl.ds(0, 12), pl.ds(0, 2)], up.at[pl.ds(0, 8), pl.ds(0, 1)])[kind % 2], corner_send.at[kind])


def solution(mesh):
    nx, ny = mesh.shape["gx"], mesh.shape["gy"]

    def local(*arrays):
        arrays = [pltpu.with_memory_space_constraint(a, pltpu.HBM) for a in arrays]
        dma = pltpu.SemaphoreType.DMA
        return pl.pallas_call(
            functools.partial(kernel, nx, ny),
            out_shape=jax.ShapeDtypeStruct((S, CX, CY, CZ), jnp.float32),
            in_specs=[pl.BlockSpec(memory_space=pltpu.HBM)] * 4,
            out_specs=pl.BlockSpec(memory_space=pltpu.VMEM),
            scratch_shapes=[
                pltpu.SMEM((S,), jnp.float32),
                pltpu.SMEM((S,), jnp.float32),
                pltpu.VMEM((S, CX + 8, CY + 4, CZ), jnp.float32),
                pltpu.VMEM((S, CX + 4, CY + 4, CZ), jnp.float32),
                pltpu.VMEM((CX + 6, CY + 2, CZ), jnp.float32),
                pltpu.VMEM((S, 2, 6, CY + 2, CZ), jnp.float32),
                pltpu.VMEM((CX + 6, CY + 2, CZ), jnp.float32),
                dma((S + 3,)), dma((2, 2)), dma((2, S, 2)), dma((2,)), dma((3, 2)),
                dma((2, 2)), dma((2, 2)), dma((3,)), dma((3,)),
                pltpu.SemaphoreType.REGULAR, pltpu.SemaphoreType.REGULAR,
            ],
            compiler_params=pltpu.CompilerParams(
                collective_id=0, has_side_effects=True, vmem_limit_bytes=44 << 20
            ),
        )(*arrays)

    placed = (P(None, "gx", "gy", None), P("gx", "gy", None), P(), P())
    return jax.shard_map(
        local, mesh=mesh, in_specs=placed, out_specs=P(None, "gx", "gy", None), check_vma=False
    )
```

```python
import functools

import jax
import jax.numpy as jnp
from jax import lax
from jax.experimental import pallas as pl
from jax.experimental.pallas import tpu as pltpu
from jax.sharding import PartitionSpec as P

S, CX, CY, CZ = 8, 64, 16, 128
MESH = pl.DeviceIdType.MESH
PASS_ON, PASS_ON_FIRST, SEND_FIRST, BEFORE_EDGES = 1, 4, 2, 2

FIRST, SECOND, HALF, UP = (4, 2), (2, 2), (3, 1), (3, 1)
OUTER, INNER = (-1, 7, 9), (0, 8)
OWN, BESIDE = (7,), (-1, 9)


def neighbours_in_z(z_sum, center):
    by_matmul = center.shape[0] * 2 // 3
    cells = center[:by_matmul].reshape(by_matmul * 8, CZ)
    high = cells.astype(jnp.bfloat16)
    low = (cells - high.astype(jnp.float32)).astype(jnp.bfloat16)
    first = jnp.dot(
        jnp.concatenate([high, low], axis=1), z_sum, preferred_element_type=jnp.float32
    ).reshape(by_matmul, 8, CZ)
    rest = center[by_matmul:]
    return jnp.concatenate([first, pltpu.roll(rest, 1, 2) + pltpu.roll(rest, CZ - 1, 2)], axis=0)


def substep(jobs, up, z_sum):
    def at(ref, where, x, n, y):
        return ref.at[pl.ds(x + where[0], n), pl.ds(y + where[1], 8)]

    centers = [at(src, where, x, n, y)[...] for src, where, _, _, x, n, y, _, _ in jobs]
    sums, done = neighbours_in_z(z_sum, jnp.concatenate(centers, axis=0)), 0
    for center, (src, where, dst, to, x, n, y, rate, decay) in zip(centers, jobs, strict=True):
        total = sums[done : done + n]
        done += n
        total = total + (at(src, where, x, n, y - 1)[...] + at(src, where, x, n, y + 1)[...])
        total = total + (at(src, where, x - 1, n, y)[...] + at(src, where, x + 1, n, y)[...])
        keep = (1.0 - 6.0 * rate) - decay * at(up, UP, x, n, y)[...]
        at(dst, to, x, n, y)[...] = keep * center + rate * total


def ones_beside():
    shape = (2 * CZ, CZ)
    z, column = (lax.broadcasted_iota(jnp.int32, shape, dim) for dim in (0, 1))
    apart = lax.rem(z - column + CZ, CZ)
    return jnp.where((apart == 1) | (apart == CZ - 1), 1.0, 0.0).astype(jnp.bfloat16)


def edges(src, where, dst, starts, between, rates, up, z_sum):
    middle = [[(between.at[s, side], (-x, 1)) for side, x in enumerate(starts)] for s in range(S)]
    for x_at, n, rows, ends in ((0, 6, OUTER, "out"), (1, 4, INNER, "in")):
        jobs = []
        for s in range(S):
            for side, x in enumerate(starts):
                source, target = (src.at[s], where), middle[s][side]
                if ends == "in":
                    source, target = target, dst(s, side)
                jobs += [(*source, *target, x + x_at, n, y, *rates[s]) for y in rows]
        substep(jobs, up, z_sum)


def kernel(
    nx, ny, x_hbm, u_hbm, d_hbm, k_hbm, out, second, up, splat, d_ref, k_ref, first, half, edge,
    load_sem, y_send, y_recv, x_send, x_recv, up_send, up_recv, corner_send, corner_recv, above, below,
):
    gx, gy = lax.axis_index("gx"), lax.axis_index("gy")

    def device(dx, dy):
        return (lax.rem(gx + dx + nx, nx), lax.rem(gy + dy + ny, ny))

    def load(s):
        return pltpu.make_async_copy(x_hbm.at[s], first.at[s, pl.ds(4, CX), pl.ds(2, CY)], load_sem.at[s])

    load_up = pltpu.make_async_copy(u_hbm, up.at[pl.ds(3, CX), pl.ds(1, CY)], load_sem.at[S])
    load_d = pltpu.make_async_copy(d_hbm, d_ref, load_sem.at[S + 1])
    load_k = pltpu.make_async_copy(k_hbm, k_ref, load_sem.at[S + 2])

    is_first, is_last = gx == 0, gx == nx - 1
    barrier = pltpu.get_barrier_semaphore()

    def signal(sem, dx, dy):
        pl.semaphore_signal(sem, inc=1, device_id=device(dx, dy), device_id_type=MESH)

    signal(barrier, 0, 1)
    signal(barrier, 0, -1)
    pl.when(jnp.logical_not(is_last))(lambda: signal(barrier, 1, 0))
    pl.when(is_first)(lambda: signal(barrier, -1, 0))
    for s in range(S):
        load(s).start()
    for copy in (load_up, load_d, load_k):
        copy.start()

    def remote(src, dst, send_sem, recv_sem, to):
        return pltpu.make_async_remote_copy(
            src_ref=src, dst_ref=dst, send_sem=send_sem, recv_sem=recv_sem,
            device_id=to, device_id_type=MESH,
        )

    both = (0, 1)
    pairs = ((0, 0), (0, 1), (1, 0), (1, 1))
    rows = ((16, 0), (2, 18))
    all_s = pl.ds(0, S)

    def y_face(r, s, d):
        buffer, planes = ((first, pl.ds(4, CX)), (second, pl.ds(4, CX - 4)))[r]
        a, b = rows[d]
        return remote(
            buffer.at[s, planes, pl.ds(a, 2)], buffer.at[s, planes, pl.ds(b, 2)],
            y_send.at[r, d], y_recv.at[r, s, d], device(0, 1 - 2 * d),
        )

    def x_face(part, d):
        a, b = ((64, 0), (4, 68))[d]
        r = (pl.ds(2, 2), pl.ds(16, 2), pl.ds(4, 12))[part]
        return remote(
            first.at[all_s, pl.ds(a, 4), r], first.at[all_s, pl.ds(b, 4), r],
            x_send.at[d], x_recv.at[part, d], device(1 - 2 * d, 0),
        )

    def up_y(d):
        a, b = ((16, 0), (1, 17))[d]
        return remote(
            up.at[pl.ds(3, CX), pl.ds(a, 1)], up.at[pl.ds(3, CX), pl.ds(b, 1)],
            up_send.at[0, d], up_recv.at[0, d], device(0, 1 - 2 * d),
        )

    def up_x(d):
        a, b = ((64, 0), (3, 67))[d]
        return remote(
            up.at[pl.ds(a, 3), pl.ds(1, CY)], up.at[pl.ds(b, 3), pl.ds(1, CY)],
            up_send.at[1, d], up_recv.at[1, d], device(1 - 2 * d, 0),
        )

    def corner(kind, side, d):
        to = device(0, 1 - 2 * d)
        sems = corner_send.at[kind], corner_recv.at[kind]
        if kind == 0:
            planes, (a, b) = pl.ds((1, 68)[side], 3), rows[d]
            return remote(first.at[all_s, planes, pl.ds(a, 2)], first.at[all_s, planes, pl.ds(b, 2)], *sems, to)
        if kind == 1:
            planes, (a, b) = pl.ds((1, 67)[side], 2), ((16, 0), (1, 17))[d]
            return remote(up.at[planes, pl.ds(a, 1)], up.at[planes, pl.ds(b, 1)], *sems, to)
        planes, (a, b) = pl.ds((1, 64)[side], 3), rows[d]
        return remote(second.at[all_s, planes, pl.ds(a, 2)], second.at[all_s, planes, pl.ds(b, 2)], *sems, to)

    def corners_arrived(kind):
        ref = (first.at[all_s, pl.ds(0, 12), pl.ds(0, 2)], up.at[pl.ds(0, 8), pl.ds(0, 1)])[kind % 2]
        pltpu.make_async_copy(ref, ref, corner_recv.at[kind]).wait()

    pl.semaphore_wait(barrier, 2 + jnp.where(is_first, 0, 1) + jnp.where(is_last, 1, 0))
    pl.when(jnp.logical_not(is_first))(lambda: signal(above, -1, 0))
    pl.when(is_last)(lambda: signal(below, 1, 0))
    load(0).wait()
    for d in both:
        y_face(0, 0, d).start()
    load_up.wait()
    for d in both:
        up_y(d).start()
    for s in range(1, S):
        load(s).wait()
        for d in both:
            y_face(0, s, d).start()

    def send_along_gx(d):
        up_x(d).start()
        for part in range(3):
            x_face(part, d).start()

    pl.when(jnp.logical_not(is_first))(lambda: send_along_gx(1))
    pl.when(jnp.logical_not(is_last))(lambda: pl.semaphore_wait(above, 1))
    send_along_gx(0)
    load_d.wait()
    load_k.wait()

    z_sum = ones_beside()

    def ahead(s, carry):
        rates = d_ref[s], k_ref[s]
        substep([(first.at[s], FIRST, half.at[s], HALF, 1, CX - 2, y, *rates) for y in OWN], up, z_sum)
        return carry

    lax.fori_loop(0, S, ahead, 0)
    for s in range(S):
        splat[0, s] = jnp.full((8, CZ), d_ref[s])
        splat[1, s] = jnp.full((8, CZ), k_ref[s])

    def middle(src, where, s, dst, to, x, n, rows):
        rates = d_ref[s], k_ref[s]
        between = half.at[s]
        substep([(src.at[s], where, between, HALF, x, n, y, *rates) for y in rows], up, z_sum)
        substep([(between, HALF, dst.at[s], to, x + 1, n - 2, y, *rates) for y in INNER], up, z_sum)

    for d in both:
        up_y(d).wait_recv()

    def pass_on():
        for d in both:
            up_x(d).wait_recv()
            x_face(0, d).wait_recv()
            x_face(1, d).wait_recv()
        for kind in both:
            for side, d in pairs:
                corner(kind, side, d).start()

    def send_down_first():
        pl.semaphore_wait(below, 1)
        send_along_gx(1)

    def round_one(s, carry):
        for d in both:
            y_face(0, s, d).wait_recv()
        middle(first, FIRST, s, second, SECOND, 1, CX - 2, BESIDE)
        for d in both:
            y_face(1, s, d).start()
        pl.when(jnp.logical_and(is_first, s == SEND_FIRST))(send_down_first)
        pl.when(s == jnp.where(is_first, PASS_ON_FIRST, PASS_ON))(pass_on)
        return carry

    lax.fori_loop(0, S, round_one, 0)

    def round_two(s, carry):
        for d in both:
            y_face(1, s, d).wait_recv()
        middle(second, SECOND, s, out, (0, 0), 3, CX - 6, OUTER)

        @pl.when(s == BEFORE_EDGES - 1)
        def _():
            for d in both:
                x_face(2, d).wait_recv()
            corners_arrived(0)
            corners_arrived(1)
            rates = [(d_ref[s], k_ref[s]) for s in range(S)]
            edges(first, FIRST, lambda s, side: (second.at[s], SECOND), (-3, CX - 3), edge, rates, up, z_sum)
            for side, d in pairs:
                corner(2, side, d).start()

        return carry

    lax.fori_loop(0, S, round_two, 0)
    corners_arrived(2)

    def sent(ref, sem):
        pltpu.make_async_copy(ref, ref, sem).wait()

    for d in both:
        sent(first.at[all_s, pl.ds(0, CX), pl.ds(0, 2)], y_send.at[0, d])
        sent(second.at[all_s, pl.ds(0, CX - 4), pl.ds(0, 2)], y_send.at[1, d])
        sent(first.at[all_s, pl.ds(0, 4), pl.ds(0, CY)], x_send.at[d])
        up_y(d).wait_send()
        up_x(d).wait_send()
    for kind in range(3):
        sent((first.at[all_s, pl.ds(0, 12), pl.ds(0, 2)], up.at[pl.ds(0, 8), pl.ds(0, 1)])[kind % 2], corner_send.at[kind])


def finish(out, second, up, splat, result, edge, rim, sem):
    inner = [pltpu.make_async_copy(out.at[s, pl.ds(4, CX - 8)], result.at[s, pl.ds(4, CX - 8)], sem.at[s]) for s in range(S)]
    outer = [
        pltpu.make_async_copy(rim.at[pl.ds(0, S), side], result.at[pl.ds(0, S), pl.ds(x, 4)], sem.at[S + side])
        for side, x in enumerate((0, CX - 4))
    ]
    for copy in inner:
        copy.start()
    rates = [(splat[0, s], splat[1, s]) for s in range(S)]
    place = ((0, 0), (4 - CX, 0))
    edges(second, SECOND, lambda s, side: (rim.at[s, side], place[side]), (-1, CX - 5), edge, rates, up, ones_beside())
    for copy in outer:
        copy.start()
    for copy in inner + outer:
        copy.wait()


def solution(mesh):
    nx, ny = mesh.shape["gx"], mesh.shape["gy"]

    def local(*arrays):
        arrays = [pltpu.with_memory_space_constraint(a, pltpu.HBM) for a in arrays]
        dma = pltpu.SemaphoreType.DMA
        f32, vmem = jnp.float32, pl.BlockSpec(memory_space=pltpu.VMEM)
        shapes = (S, CX, CY, CZ), (S, CX + 4, CY + 4, CZ), (CX + 6, CY + 2, CZ), (2, S, 8, CZ)
        between = pltpu.VMEM((S, 2, 6, CY + 2, CZ), f32)
        parts = pl.pallas_call(
            functools.partial(kernel, nx, ny),
            out_shape=[jax.ShapeDtypeStruct(shape, f32) for shape in shapes],
            in_specs=[pl.BlockSpec(memory_space=pltpu.HBM)] * 4,
            out_specs=[vmem] * 4,
            scratch_shapes=[
                pltpu.SMEM((S,), f32),
                pltpu.SMEM((S,), f32),
                pltpu.VMEM((S, CX + 8, CY + 4, CZ), f32),
                pltpu.VMEM((S, CX + 6, CY + 2, CZ), f32),
                between,
                dma((S + 3,)), dma((2, 2)), dma((2, S, 2)), dma((2,)), dma((3, 2)),
                dma((2, 2)), dma((2, 2)), dma((3,)), dma((3,)),
                pltpu.SemaphoreType.REGULAR, pltpu.SemaphoreType.REGULAR,
            ],
            compiler_params=pltpu.CompilerParams(
                collective_id=0, has_side_effects=True, vmem_limit_bytes=40 << 20
            ),
        )(*arrays)
        return pl.pallas_call(
            finish,
            out_shape=jax.ShapeDtypeStruct(shapes[0], f32),
            in_specs=[vmem] * 4,
            out_specs=pl.BlockSpec(memory_space=pltpu.HBM),
            scratch_shapes=[between, pltpu.VMEM((S, 2, 4, CY, CZ), f32), dma((S + 2,))],
            compiler_params=pltpu.CompilerParams(vmem_limit_bytes=32 << 20),
        )(*parts)

    placed = (P(None, "gx", "gy", None), P("gx", "gy", None), P(), P())
    return jax.shard_map(
        local, mesh=mesh, in_specs=placed, out_specs=P(None, "gx", "gy", None), check_vma=False
    )
```

```python
import functools

import jax
import jax.numpy as jnp
from jax import lax
from jax.experimental import pallas as pl
from jax.experimental.pallas import tpu as pltpu
from jax.sharding import PartitionSpec as P

S, CX, CY, CZ = 8, 64, 16, 128
MESH = pl.DeviceIdType.MESH
PASS_ON, PASS_ON_FIRST, SEND_FIRST, BEFORE_EDGES, BEFORE_EDGES_FIRST = 2, 4, 2, 1, 2

FIRST, SECOND, HALF, UP = (4, 2), (2, 2), (3, 1), (3, 1)
OUTER, INNER = (-1, 7, 9), (0, 8)
CHUNK = 1
OWN, BESIDE = (7,), (-1, 9)


def neighbours_in_z(z_sum, center):
    by_matmul = center.shape[0] * 2 // 3
    cells = center[:by_matmul].reshape(by_matmul * 8, CZ)
    high = cells.astype(jnp.bfloat16)
    low = (cells - high.astype(jnp.float32)).astype(jnp.bfloat16)
    first = jnp.dot(
        jnp.concatenate([high, low], axis=1), z_sum, preferred_element_type=jnp.float32
    ).reshape(by_matmul, 8, CZ)
    rest = center[by_matmul:]
    return jnp.concatenate([first, pltpu.roll(rest, 1, 2) + pltpu.roll(rest, CZ - 1, 2)], axis=0)


def substep(jobs, up, z_sum):
    def at(ref, where, x, n, y):
        return ref.at[pl.ds(x + where[0], n), pl.ds(y + where[1], 8)]

    centers = [at(src, where, x, n, y)[...] for src, where, _, _, x, n, y, _, _ in jobs]
    sums, done = neighbours_in_z(z_sum, jnp.concatenate(centers, axis=0)), 0
    for src, where, dst, to, first, planes, y, rate, decay in jobs:
        stay = 1.0 - 6.0 * rate
        for x in range(first, first + planes, CHUNK):
            n = min(CHUNK, first + planes - x)
            total = sums[done : done + n]
            done += n
            total = total + (at(src, where, x, n, y - 1)[...] + at(src, where, x, n, y + 1)[...])
            total = total + (at(src, where, x - 1, n, y)[...] + at(src, where, x + 1, n, y)[...])
            keep = stay - decay * at(up, UP, x, n, y)[...]
            at(dst, to, x, n, y)[...] = keep * at(src, where, x, n, y)[...] + rate * total


def ones_beside():
    shape = (2 * CZ, CZ)
    z, column = (lax.broadcasted_iota(jnp.int32, shape, dim) for dim in (0, 1))
    apart = lax.rem(z - column + CZ, CZ)
    return jnp.where((apart == 1) | (apart == CZ - 1), 1.0, 0.0).astype(jnp.bfloat16)


def edges(src, where, dst, starts, between, rates, up, z_sum):
    middle = [[(between.at[s, side], (-x, 1)) for side, x in enumerate(starts)] for s in range(S)]
    for x_at, n, rows, ends in ((0, 6, OUTER, "out"), (1, 4, INNER, "in")):
        jobs = []
        for s in range(S):
            for side, x in enumerate(starts):
                source, target = (src.at[s], where), middle[s][side]
                if ends == "in":
                    source, target = target, dst(s, side)
                jobs += [(*source, *target, x + x_at, n, y, *rates[s]) for y in rows]
        substep(jobs, up, z_sum)


def kernel(
    nx, ny, x_hbm, u_hbm, d_hbm, k_hbm, out, second, up, splat, d_ref, k_ref, first, half, edge,
    load_sem, y_send, y_recv, x_send, x_recv, up_send, up_recv, corner_send, corner_recv, above, below,
):
    gx, gy = lax.axis_index("gx"), lax.axis_index("gy")

    def device(dx, dy):
        return (lax.rem(gx + dx + nx, nx), lax.rem(gy + dy + ny, ny))

    def load(s):
        return pltpu.make_async_copy(x_hbm.at[s], first.at[s, pl.ds(4, CX), pl.ds(2, CY)], load_sem.at[s])

    load_up = pltpu.make_async_copy(u_hbm, up.at[pl.ds(3, CX), pl.ds(1, CY)], load_sem.at[S])
    load_d = pltpu.make_async_copy(d_hbm, d_ref, load_sem.at[S + 1])
    load_k = pltpu.make_async_copy(k_hbm, k_ref, load_sem.at[S + 2])

    is_first, is_last = gx == 0, gx == nx - 1
    barrier = pltpu.get_barrier_semaphore()

    def signal(sem, dx, dy):
        pl.semaphore_signal(sem, inc=1, device_id=device(dx, dy), device_id_type=MESH)

    signal(barrier, 0, 1)
    signal(barrier, 0, -1)
    pl.when(jnp.logical_not(is_last))(lambda: signal(barrier, 1, 0))
    pl.when(is_first)(lambda: signal(barrier, -1, 0))
    for s in range(S):
        load(s).start()
    for copy in (load_up, load_d, load_k):
        copy.start()

    def remote(src, dst, send_sem, recv_sem, to):
        return pltpu.make_async_remote_copy(
            src_ref=src, dst_ref=dst, send_sem=send_sem, recv_sem=recv_sem,
            device_id=to, device_id_type=MESH,
        )

    both = (0, 1)
    pairs = ((0, 0), (0, 1), (1, 0), (1, 1))
    rows = ((16, 0), (2, 18))
    all_s = pl.ds(0, S)

    def y_face(r, s, d):
        buffer, planes = ((first, pl.ds(4, CX)), (second, pl.ds(4, CX - 4)))[r]
        a, b = rows[d]
        return remote(
            buffer.at[s, planes, pl.ds(a, 2)], buffer.at[s, planes, pl.ds(b, 2)],
            y_send.at[r, d], y_recv.at[r, s, d], device(0, 1 - 2 * d),
        )

    def x_face(part, d):
        a, b = ((64, 0), (4, 68))[d]
        r = (pl.ds(2, 2), pl.ds(16, 2), pl.ds(4, 12))[part]
        return remote(
            first.at[all_s, pl.ds(a, 4), r], first.at[all_s, pl.ds(b, 4), r],
            x_send.at[d], x_recv.at[part, d], device(1 - 2 * d, 0),
        )

    def up_y(d):
        a, b = ((16, 0), (1, 17))[d]
        return remote(
            up.at[pl.ds(3, CX), pl.ds(a, 1)], up.at[pl.ds(3, CX), pl.ds(b, 1)],
            up_send.at[0, d], up_recv.at[0, d], device(0, 1 - 2 * d),
        )

    def up_x(d):
        a, b = ((64, 0), (3, 67))[d]
        return remote(
            up.at[pl.ds(a, 3), pl.ds(1, CY)], up.at[pl.ds(b, 3), pl.ds(1, CY)],
            up_send.at[1, d], up_recv.at[1, d], device(1 - 2 * d, 0),
        )

    def corner(kind, side, d):
        to = device(0, 1 - 2 * d)
        sems = corner_send.at[kind], corner_recv.at[kind]
        if kind == 0:
            planes, (a, b) = pl.ds((1, 68)[side], 3), rows[d]
            return remote(first.at[all_s, planes, pl.ds(a, 2)], first.at[all_s, planes, pl.ds(b, 2)], *sems, to)
        if kind == 1:
            planes, (a, b) = pl.ds((1, 67)[side], 2), ((16, 0), (1, 17))[d]
            return remote(up.at[planes, pl.ds(a, 1)], up.at[planes, pl.ds(b, 1)], *sems, to)
        planes, (a, b) = pl.ds((1, 64)[side], 3), rows[d]
        return remote(second.at[all_s, planes, pl.ds(a, 2)], second.at[all_s, planes, pl.ds(b, 2)], *sems, to)

    def corners_arrived(kind):
        ref = (first.at[all_s, pl.ds(0, 12), pl.ds(0, 2)], up.at[pl.ds(0, 8), pl.ds(0, 1)])[kind % 2]
        pltpu.make_async_copy(ref, ref, corner_recv.at[kind]).wait()

    pl.semaphore_wait(barrier, 2 + jnp.where(is_first, 0, 1) + jnp.where(is_last, 1, 0))
    pl.when(jnp.logical_not(is_first))(lambda: signal(above, -1, 0))
    pl.when(is_last)(lambda: signal(below, 1, 0))
    load(0).wait()
    for d in both:
        y_face(0, 0, d).start()
    load_up.wait()
    for d in both:
        up_y(d).start()
    for s in range(1, S):
        load(s).wait()
        for d in both:
            y_face(0, s, d).start()

    def send_along_gx(d):
        up_x(d).start()
        for part in range(3):
            x_face(part, d).start()

    pl.when(jnp.logical_not(is_first))(lambda: send_along_gx(1))
    pl.when(jnp.logical_not(is_last))(lambda: pl.semaphore_wait(above, 1))
    send_along_gx(0)
    load_d.wait()
    load_k.wait()

    z_sum = ones_beside()

    def ahead(s, carry):
        rates = d_ref[s], k_ref[s]
        substep([(first.at[s], FIRST, half.at[s], HALF, 1, CX - 2, y, *rates) for y in OWN], up, z_sum)
        return carry

    lax.fori_loop(0, S, ahead, 0)
    for s in range(S):
        splat[0, s] = jnp.full((8, CZ), d_ref[s])
        splat[1, s] = jnp.full((8, CZ), k_ref[s])

    def one(src, where, s, x, n, rows):
        return [(src.at[s], where, half.at[s], HALF, x, n, y, d_ref[s], k_ref[s]) for y in rows]

    def two(s, dst, to, x, n):
        return [(half.at[s], HALF, dst.at[s], to, x, n, y, d_ref[s], k_ref[s]) for y in INNER]

    one_first = lambda s: one(first, FIRST, s, 1, CX - 2, BESIDE)
    two_first = lambda s: two(s, second, SECOND, 2, CX - 4)
    one_second = lambda s: one(second, SECOND, s, 3, CX - 6, OUTER)
    two_second = lambda s: two(s, out, (0, 0), 4, CX - 8)

    for d in both:
        up_y(d).wait_recv()

    def pass_on():
        for d in both:
            up_x(d).wait_recv()
            x_face(0, d).wait_recv()
            x_face(1, d).wait_recv()
        for kind in both:
            for side, d in pairs:
                corner(kind, side, d).start()

    def send_down_first():
        pl.semaphore_wait(below, 1)
        send_along_gx(1)

    def arrived(r, s):
        for d in both:
            y_face(r, s, d).wait_recv()

    def send_second(s):
        for d in both:
            y_face(1, s, d).start()

    def round_one(s, carry):
        arrived(0, s)
        substep(two_first(s - 1) + one_first(s), up, z_sum)
        send_second(s - 1)
        pl.when(jnp.logical_and(is_first, s == SEND_FIRST))(send_down_first)
        pl.when(s == jnp.where(is_first, PASS_ON_FIRST, PASS_ON))(pass_on)
        return carry

    arrived(0, 0)
    substep(one_first(0), up, z_sum)
    lax.fori_loop(1, S, round_one, 0)
    substep(two_first(S - 1), up, z_sum)
    send_second(S - 1)

    def edges_between():
        for d in both:
            x_face(2, d).wait_recv()
        corners_arrived(0)
        corners_arrived(1)
        rates = [(d_ref[s], k_ref[s]) for s in range(S)]
        edges(first, FIRST, lambda s, side: (second.at[s], SECOND), (-3, CX - 3), edge, rates, up, z_sum)
        for side, d in pairs:
            corner(2, side, d).start()

    def round_two(s, carry):
        arrived(1, s)
        substep(two_second(s - 1) + one_second(s), up, z_sum)
        pl.when(s == jnp.where(is_first, BEFORE_EDGES_FIRST, BEFORE_EDGES))(edges_between)
        return carry

    arrived(1, 0)
    substep(one_second(0), up, z_sum)
    lax.fori_loop(1, S, round_two, 0)
    substep(two_second(S - 1), up, z_sum)
    corners_arrived(2)

    def sent(ref, sem):
        pltpu.make_async_copy(ref, ref, sem).wait()

    for d in both:
        sent(first.at[all_s, pl.ds(0, CX), pl.ds(0, 2)], y_send.at[0, d])
        sent(second.at[all_s, pl.ds(0, CX - 4), pl.ds(0, 2)], y_send.at[1, d])
        sent(first.at[all_s, pl.ds(0, 4), pl.ds(0, CY)], x_send.at[d])
        up_y(d).wait_send()
        up_x(d).wait_send()
    for kind in range(3):
        sent((first.at[all_s, pl.ds(0, 12), pl.ds(0, 2)], up.at[pl.ds(0, 8), pl.ds(0, 1)])[kind % 2], corner_send.at[kind])


def finish(out, second, up, splat, result, edge, rim, sem):
    inner = [pltpu.make_async_copy(out.at[s, pl.ds(4, CX - 8)], result.at[s, pl.ds(4, CX - 8)], sem.at[s]) for s in range(S)]
    outer = [
        pltpu.make_async_copy(rim.at[pl.ds(0, S), side], result.at[pl.ds(0, S), pl.ds(x, 4)], sem.at[S + side])
        for side, x in enumerate((0, CX - 4))
    ]
    for copy in inner:
        copy.start()
    rates = [(splat[0, s], splat[1, s]) for s in range(S)]
    place = ((0, 0), (4 - CX, 0))
    edges(second, SECOND, lambda s, side: (rim.at[s, side], place[side]), (-1, CX - 5), edge, rates, up, ones_beside())
    for copy in outer:
        copy.start()
    for copy in inner + outer:
        copy.wait()


def solution(mesh):
    nx, ny = mesh.shape["gx"], mesh.shape["gy"]

    def local(*arrays):
        arrays = [pltpu.with_memory_space_constraint(a, pltpu.HBM) for a in arrays]
        dma = pltpu.SemaphoreType.DMA
        f32, vmem = jnp.float32, pl.BlockSpec(memory_space=pltpu.VMEM)
        shapes = (S, CX, CY, CZ), (S, CX + 4, CY + 4, CZ), (CX + 6, CY + 2, CZ), (2, S, 8, CZ)
        between = pltpu.VMEM((S, 2, 6, CY + 2, CZ), f32)
        parts = pl.pallas_call(
            functools.partial(kernel, nx, ny),
            out_shape=[jax.ShapeDtypeStruct(shape, f32) for shape in shapes],
            in_specs=[pl.BlockSpec(memory_space=pltpu.HBM)] * 4,
            out_specs=[vmem] * 4,
            scratch_shapes=[
                pltpu.SMEM((S,), f32),
                pltpu.SMEM((S,), f32),
                pltpu.VMEM((S, CX + 8, CY + 4, CZ), f32),
                pltpu.VMEM((S, CX + 6, CY + 2, CZ), f32),
                between,
                dma((S + 3,)), dma((2, 2)), dma((2, S, 2)), dma((2,)), dma((3, 2)),
                dma((2, 2)), dma((2, 2)), dma((3,)), dma((3,)),
                pltpu.SemaphoreType.REGULAR, pltpu.SemaphoreType.REGULAR,
            ],
            compiler_params=pltpu.CompilerParams(
                collective_id=0, has_side_effects=True, vmem_limit_bytes=40 << 20
            ),
        )(*arrays)
        return pl.pallas_call(
            finish,
            out_shape=jax.ShapeDtypeStruct(shapes[0], f32),
            in_specs=[vmem] * 4,
            out_specs=pl.BlockSpec(memory_space=pltpu.HBM),
            scratch_shapes=[between, pltpu.VMEM((S, 2, 4, CY, CZ), f32), dma((S + 2,))],
            compiler_params=pltpu.CompilerParams(vmem_limit_bytes=32 << 20),
        )(*parts)

    placed = (P(None, "gx", "gy", None), P("gx", "gy", None), P(), P())
    return jax.shard_map(
        local, mesh=mesh, in_specs=placed, out_specs=P(None, "gx", "gy", None), check_vma=False
    )
```
